32 devices in a mesh: row: 4 (over z), col: 8 (over y, x, core).
Axes of the slice: x: 2, y: 2, z: 4, core: 2. Of those that a mesh axis runs over, the one named last changes fastest.
Arguments:
- grad: float32 [8192, 14336], P(('row', 'col')), may hold values from -30 to 30
- momentum: float32 [8192, 14336], P(('row', 'col')), may hold values from -6 to 6
- weight: float32 [8192, 14336], P(('row', 'col')), may hold values from -0.75 to 0.75
Outputs:
- new_weight: float32 [8192, 14336], P('row', 'col')
- new_momentum: float32 [8192, 14336], P('row', 'col')
The draws below stay inside these ranges and needn't reach their ends.
All inputs are finite; a program needn't handle non-finite values.
Results may differ from the reference program's by a relative error of at most 0.00002.
Values sent between devices are 32-bit elements; how exact they have to be, the bound alone decides.
A program may use at most 192 MiB of HBM per device.

```python
import math
import jax
import jax.numpy as jnp

D = 8192
FF = 14336


def draw_grad(key, part):
    key_rows, key_cols, key_base = jax.random.split(key, 3)
    row_scale = jnp.exp(jax.random.uniform(key_rows, (D, 1), jnp.float32) * jnp.log(10.0))
    col_scale = jnp.exp(jax.random.uniform(key_cols, (1, FF), jnp.float32) * jnp.log(10.0))
    ramp = 1.0 + 2.0 * jnp.arange(D, dtype=jnp.float32).reshape(D, 1) / (D - 1)
    base = jnp.clip(jax.random.normal(key_base, (D, FF), jnp.float32), -6.0, 6.0)
    scaled = base * row_scale * col_scale * ramp / 10.0
    return jnp.clip(scaled, -30.0, 30.0).astype(jnp.float32)


def levels(stream_key, extent, shards, low, high):
    level, own = 1.0, jax.random.fold_in(stream_key, 6)
    for position, shards_of in shards:
        draws = jnp.exp(jax.random.uniform(jax.random.fold_in(own, position), (shards_of,), jnp.float32, low / len(shards), high / len(shards)))
        level = level * jnp.repeat(draws, extent[position] // shards_of).reshape([-1 if axis == position else 1 for axis in range(len(extent))])
    return level


def gaussian(rng, shape, deviation, bound, shards=(), held_as=jnp.bfloat16):
    loudness = levels(rng, shape, shards, -0.22, 0.18) if shards else 1.0
    drawn = jax.random.normal(rng, shape, jnp.float32) * deviation * loudness
    return jnp.minimum(jnp.maximum(drawn, -bound), bound).astype(held_as)


def setup_inputs(seed: int = 0) -> dict:
    seeds = jax.random.split(jax.random.key(seed), 4)
    return {
        "grad": draw_grad(jax.random.fold_in(seeds[3], 71), 0),
        "momentum": gaussian(seeds[1], (D, FF), 1.0, 6.0, ((0, 32),), jnp.float32),
        "weight": gaussian(seeds[2], (D, FF), 0.05, 0.75, ((0, 32),), jnp.float32),
    }


def reference(grad, momentum, weight):
    total = jnp.sum(grad * grad)
    limit = jnp.float32(math.sqrt(D * FF))
    factor = jnp.minimum(jnp.float32(1.0), limit / (jnp.sqrt(total) + jnp.float32(1e-06)))
    new_momentum = jnp.float32(0.9) * momentum + factor * grad
    new_weight = weight - jnp.float32(0.1) * new_momentum
    return (new_weight, new_momentum)
```

```python
import functools
import math

import jax
import jax.numpy as jnp
from jax import lax
from jax.experimental import pallas as pl
from jax.experimental.pallas import tpu as pltpu
from jax.sharding import PartitionSpec as P

F32 = jnp.float32
MESH = pl.DeviceIdType.MESH
MIB = 1 << 20


def partner(me, k, n):
    if n & (n - 1):
        return lax.rem(me + k, n)
    index, bit = 0, 1
    while bit < n:
        own = lax.rem(me // bit, 2)
        index = index + (1 - own if k & bit else own) * bit
        bit *= 2
    return index


def source(me, k, n):
    return lax.rem(me + n - k, n) if n & (n - 1) else partner(me, k, n)


def exchange(
    n, nr, limit, head, step,
    g_ref, m_ref, w_ref, w_out, nm_out,
    gbuf, mbuf, part, col_parts, row_parts,
    g_sem, m_sem, own_sem, w_send, w_recv, nm_send, nm_recv, cs_sem, cr_sem, rs_sem, rr_sem,
):
    rows, width = g_ref.shape
    cols = width // n
    me, me_row = lax.axis_index("col"), lax.axis_index("row")
    chunks = rows // step

    def window(index):
        return pl.ds(pl.multiple_of(index * cols, 128), cols)

    def landing(index, start, size):
        return pl.ds(pl.multiple_of(index * rows + start, 8), size)

    def piece(src, dst, to, frm, start, size, send, recv, k, part_index):
        out = pltpu.make_async_remote_copy(
            src_ref=src.at[pl.ds(start, size), window(to)],
            dst_ref=dst.at[landing(me, start, size), :],
            send_sem=send.at[k, part_index], recv_sem=recv.at[k, part_index],
            device_id={"col": to}, device_id_type=MESH,
        )
        arriving = pltpu.make_async_remote_copy(
            src_ref=src.at[pl.ds(start, size), window(to)],
            dst_ref=dst.at[landing(frm, start, size), :],
            send_sem=send.at[k, part_index], recv_sem=recv.at[k, part_index],
            device_id={"col": to}, device_id_type=MESH,
        )
        return out, arriving

    peers = {k: (partner(me, k, n), source(me, k, n)) for k in range(1, n)}
    near = [k for k in peers if k >> 1 == 0]
    direct = [k for k in peers if k >> 1 and not (k >> 1) & ((k >> 1) - 1)]
    routed = [k for k in peers if k not in near and k not in direct]

    g_loads = [
        pltpu.make_async_copy(g_ref.at[pl.ds(c * step, step)], gbuf.at[pl.ds(c * step, step)], g_sem.at[c])
        for c in range(chunks)
    ]
    for load in g_loads:
        load.start()

    def m_load(c):
        return pltpu.make_async_copy(m_ref.at[pl.ds(c * step, step)], mbuf.at[c % 2], m_sem.at[c % 2])

    barrier = pltpu.get_barrier_semaphore()
    for k in peers:
        pl.semaphore_signal(barrier, inc=1, device_id={"col": peers[k][0]}, device_id_type=MESH)
    for k in range(1, nr):
        pl.semaphore_signal(barrier, inc=1, device_id={"row": partner(me_row, k, nr)}, device_id_type=MESH)
    pl.semaphore_wait(barrier, n - 1 + nr - 1)

    w_first = {k: piece(w_ref, w_out, *peers[k], 0, head, w_send, w_recv, k, 0) for k in peers}
    w_rest = {k: piece(w_ref, w_out, *peers[k], head, rows - head, w_send, w_recv, k, 1) for k in peers}
    nm_all = {k: piece(gbuf, nm_out, *peers[k], 0, rows, nm_send, nm_recv, k, 0) for k in peers}

    for k in direct:
        w_first[k][0].start()

    total = jnp.zeros((8, cols), F32)
    for c in range(chunks):
        g_loads[c].wait()

        def add(r, total, c=c):
            start = pl.multiple_of(c * step + r * 8, 8)
            for p in range(n):
                x = gbuf[pl.ds(start, 8), pl.ds(p * cols, cols)]
                total = total + x * x
            return total

        total = lax.fori_loop(0, step // 8, add, total)
    tile = total[:, 0:128]
    for p in range(1, cols // 128):
        tile = tile + total[:, p * 128 : (p + 1) * 128]
    part[...] = tile
    col_parts[me] = tile

    for c in range(2):
        m_load(c).start()
    own_w = pltpu.make_async_copy(w_ref.at[:, window(me)], w_out.at[landing(me, 0, rows), :], own_sem.at[0])
    own_w.start()

    def col_share(k, slot):
        return pltpu.make_async_remote_copy(
            src_ref=part, dst_ref=col_parts.at[slot], send_sem=cs_sem.at[k], recv_sem=cr_sem.at[k],
            device_id={"col": peers[k][0]}, device_id_type=MESH,
        )

    for k in peers:
        col_share(k, me).start()

    for k in direct:
        w_rest[k][0].start()
    for k in routed:
        w_rest[k][0].start()
    for k in routed:
        w_first[k][0].start()
    for k in near:
        w_first[k][0].start()
        w_rest[k][0].start()

    for k in peers:
        col_share(k, peers[k][1]).wait_recv()

    def row_share(k, slot):
        return pltpu.make_async_remote_copy(
            src_ref=col_parts, dst_ref=row_parts.at[slot], send_sem=rs_sem.at[k], recv_sem=rr_sem.at[k],
            device_id={"row": partner(me_row, k, nr)}, device_id_type=MESH,
        )

    for k in range(1, nr):
        row_share(k, me_row).start()
    row_parts[me_row] = col_parts[...]
    for k in range(1, nr):
        row_share(k, source(me_row, k, nr)).wait_recv()

    square = jnp.sum(row_parts[...].reshape(nr * n * 8, 128), keepdims=True)
    factor = jnp.minimum(F32(1.0), F32(limit) / (jnp.sqrt(square) + F32(1e-06)))
    factor = jnp.broadcast_to(factor, (8, cols))

    for c in range(chunks):
        m_load(c).wait()

        def update(r, carry, c=c):
            start = pl.multiple_of(c * step + r * 8, 8)
            for p in range(n):
                span = pl.ds(p * cols, cols)
                m = mbuf[c % 2, pl.ds(pl.multiple_of(r * 8, 8), 8), span]
                gbuf[pl.ds(start, 8), span] = F32(0.9) * m + factor * gbuf[pl.ds(start, 8), span]
            return carry

        lax.fori_loop(0, step // 8, update, 0)
        if c + 2 < chunks:
            m_load(c + 2).start()

    for k in routed:
        w_rest[k][0].wait_send()
    for k in direct + routed + near:
        nm_all[k][0].start()
    own_nm = pltpu.make_async_copy(gbuf.at[:, window(me)], nm_out.at[landing(me, 0, rows), :], own_sem.at[1])
    own_nm.start()

    for k in peers:
        w_first[k][0].wait_send()
        if k not in routed:
            w_rest[k][0].wait_send()
        col_share(k, me).wait_send()
    for k in range(1, nr):
        row_share(k, me_row).wait_send()
    own_w.wait()
    own_nm.wait()
    for k in peers:
        w_first[k][1].wait_recv()
        w_rest[k][1].wait_recv()
    for k in peers:
        nm_all[k][0].wait_send()
        nm_all[k][1].wait_recv()


def finish(block, w_ref, nm_ref, nw_out, nm_out, buf, nw_sem, nm_sem):
    rows = w_ref.shape[0]
    blocks = rows // block
    whole = pltpu.make_async_copy(nm_ref, nm_out, nm_sem)

    def write(b):
        return pltpu.make_async_copy(buf.at[b], nw_out.at[pl.ds(b * block, block)], nw_sem.at[b])

    for b in range(blocks):
        if b == 1:
            whole.start()

        def step(r, carry, b=b):
            start = pl.multiple_of(b * block + r * 8, 8)
            buf[b, pl.ds(pl.multiple_of(r * 8, 8), 8)] = w_ref[pl.ds(start, 8)] - F32(0.1) * nm_ref[pl.ds(start, 8)]
            return carry

        lax.fori_loop(0, block // 8, step, 0)
        write(b).start()
    whole.wait()
    for b in range(blocks):
        write(b).wait()


def body(n, nr, grad, momentum, weight):
    rows, width = grad.shape
    cols = width // n
    limit = math.sqrt(rows * n * nr * width)
    head = max(8, rows // 64 * 8)
    step = max(8, rows // 64 * 8)
    dma = pltpu.SemaphoreType.DMA
    anywhere, vmem = pl.BlockSpec(memory_space=pl.ANY), pl.BlockSpec(memory_space=pltpu.VMEM)
    local = rows * width * 4
    w_new, nm_new = pl.pallas_call(
        functools.partial(exchange, n, nr, limit, head, step),
        out_shape=(pltpu.VMEM((n * rows, cols), F32),) * 2,
        in_specs=[anywhere] * 3,
        out_specs=(vmem,) * 2,
        scratch_shapes=[
            pltpu.VMEM((rows, width), F32),
            pltpu.VMEM((2, step, width), F32),
            pltpu.VMEM((8, 128), F32),
            pltpu.VMEM((n, 8, 128), F32),
            pltpu.VMEM((nr, n, 8, 128), F32),
            dma((rows // step,)), dma((2,)), dma((2,)),
            dma((n, 2)), dma((n, 2)), dma((n, 1)), dma((n, 1)),
            dma((n,)), dma((n,)), dma((nr,)), dma((nr,)),
        ],
        compiler_params=pltpu.CompilerParams(
            collective_id=0, has_side_effects=True,
            vmem_limit_bytes=local + 2 * step * width * 4 + 2 * MIB,
        ),
        name="exchange",
    )(grad, momentum, weight)
    block = n * rows // 16
    return pl.pallas_call(
        functools.partial(finish, block),
        out_shape=(jax.ShapeDtypeStruct((n * rows, cols), F32),) * 2,
        in_specs=[vmem] * 2,
        out_specs=(anywhere,) * 2,
        scratch_shapes=[pltpu.VMEM((16, block, cols), F32), dma((16,)), dma],
        compiler_params=pltpu.CompilerParams(vmem_limit_bytes=local + 2 * MIB),
        name="finish",
    )(w_new, nm_new)


def solution(mesh):
    n, nr = mesh.shape["col"], mesh.shape["row"]
    spread = P(("row", "col"), None)
    return jax.shard_map(
        functools.partial(body, n, nr),
        mesh=mesh,
        in_specs=(spread,) * 3,
        out_specs=(P("row", "col"),) * 2,
        check_vma=False,
    )
```

```python
import functools
import math

import jax
import jax.numpy as jnp
from jax import lax
from jax.experimental import pallas as pl
from jax.experimental.pallas import tpu as pltpu
from jax.sharding import PartitionSpec as P

F32 = jnp.float32
MESH = pl.DeviceIdType.MESH
MIB = 1 << 20
TAIL = 32


def partner(me, k, n):
    if n & (n - 1):
        return lax.rem(me + k, n)
    index, bit = 0, 1
    while bit < n:
        own = lax.rem(me // bit, 2)
        index = index + (1 - own if k & bit else own) * bit
        bit *= 2
    return index


def source(me, k, n):
    return lax.rem(me + n - k, n) if n & (n - 1) else partner(me, k, n)


def kinds(n):
    near = [1] if n > 1 else []
    direct = [k for k in range(2, n) if not (k >> 1) & ((k >> 1) - 1)]
    return near, direct, [k for k in range(2, n) if k not in direct]


def exchange(
    n, nr, limit, head, step, tail,
    g_ref, m_ref, w_ref, w_out, nm_out, *refs,
):
    near, direct, routed = kinds(n)
    tail_outs, refs = refs[: len(direct)], refs[len(direct) :]
    exchange_body(n, nr, limit, head, step, tail, g_ref, m_ref, w_ref, w_out, nm_out, tail_outs, *refs)


def exchange_body(
    n, nr, limit, head, step, tail,
    g_ref, m_ref, w_ref, w_out, nm_out, tail_outs,
    gbuf, mbuf, part, col_parts, row_parts,
    g_sem, m_sem, own_sem, tail_sem, w_send, w_recv, nm_send, nm_recv, cs_sem, cr_sem, rs_sem, rr_sem,
):
    rows, width = g_ref.shape
    cols = width // n
    me, me_row = lax.axis_index("col"), lax.axis_index("row")
    chunks = rows // step

    def window(index):
        return pl.ds(pl.multiple_of(index * cols, 128), cols)

    def landing(index, start, size):
        return pl.ds(pl.multiple_of(index * rows + start, 8), size)

    def piece(src, dst, to, frm, start, size, send, recv, k, part_index):
        out = pltpu.make_async_remote_copy(
            src_ref=src.at[pl.ds(start, size), window(to)],
            dst_ref=dst.at[landing(me, start, size), :],
            send_sem=send.at[k, part_index], recv_sem=recv.at[k, part_index],
            device_id={"col": to}, device_id_type=MESH,
        )
        arriving = pltpu.make_async_remote_copy(
            src_ref=src.at[pl.ds(start, size), window(to)],
            dst_ref=dst.at[landing(frm, start, size), :],
            send_sem=send.at[k, part_index], recv_sem=recv.at[k, part_index],
            device_id={"col": to}, device_id_type=MESH,
        )
        return out, arriving

    peers = {k: (partner(me, k, n), source(me, k, n)) for k in range(1, n)}
    near, direct, routed = kinds(n)

    g_loads = [
        pltpu.make_async_copy(g_ref.at[pl.ds(c * step, step)], gbuf.at[pl.ds(c * step, step)], g_sem.at[c])
        for c in range(chunks)
    ]
    for load in g_loads:
        load.start()

    def m_load(c):
        return pltpu.make_async_copy(m_ref.at[pl.ds(c * step, step)], mbuf.at[c % 2], m_sem.at[c % 2])

    barrier = pltpu.get_barrier_semaphore()
    for k in peers:
        pl.semaphore_signal(barrier, inc=1, device_id={"col": peers[k][0]}, device_id_type=MESH)
    for k in range(1, nr):
        pl.semaphore_signal(barrier, inc=1, device_id={"row": partner(me_row, k, nr)}, device_id_type=MESH)
    pl.semaphore_wait(barrier, n - 1 + nr - 1)

    w_first = {k: piece(w_ref, w_out, *peers[k], 0, head, w_send, w_recv, k, 0) for k in peers}
    w_rest = {k: piece(w_ref, w_out, *peers[k], head, rows - head - (tail if k in direct else 0), w_send, w_recv, k, 1) for k in peers}
    nm_all = {k: piece(gbuf, nm_out, *peers[k], 0, rows, nm_send, nm_recv, k, 0) for k in peers}

    for k in direct:
        w_first[k][0].start()

    total = jnp.zeros((8, cols), F32)
    for c in range(chunks):
        g_loads[c].wait()

        def add(r, total, c=c):
            start = pl.multiple_of(c * step + r * 8, 8)
            for p in range(n):
                x = gbuf[pl.ds(start, 8), pl.ds(p * cols, cols)]
                total = total + x * x
            return total

        total = lax.fori_loop(0, step // 8, add, total)
    tile = total[:, 0:128]
    for p in range(1, cols // 128):
        tile = tile + total[:, p * 128 : (p + 1) * 128]
    part[...] = tile
    col_parts[me] = tile

    for c in range(2):
        m_load(c).start()
    own_w = pltpu.make_async_copy(w_ref.at[:, window(me)], w_out.at[landing(me, 0, rows), :], own_sem.at[0])
    own_w.start()
    tails = [
        pltpu.make_async_copy(w_ref.at[pl.ds(rows - tail, tail), window(peers[k][0])], out, tail_sem.at[i])
        for i, (k, out) in enumerate(zip(direct, tail_outs))
    ]

    def col_share(k, slot):
        return pltpu.make_async_remote_copy(
            src_ref=part, dst_ref=col_parts.at[slot], send_sem=cs_sem.at[k], recv_sem=cr_sem.at[k],
            device_id={"col": peers[k][0]}, device_id_type=MESH,
        )

    for k in peers:
        col_share(k, me).start()

    for k in direct:
        w_rest[k][0].start()
    for k in routed:
        w_rest[k][0].start()
    for k in routed:
        w_first[k][0].start()
    for k in near:
        w_first[k][0].start()
        w_rest[k][0].start()

    for k in peers:
        col_share(k, peers[k][1]).wait_recv()

    def row_share(k, slot):
        return pltpu.make_async_remote_copy(
            src_ref=col_parts, dst_ref=row_parts.at[slot], send_sem=rs_sem.at[k], recv_sem=rr_sem.at[k],
            device_id={"row": partner(me_row, k, nr)}, device_id_type=MESH,
        )

    for k in range(1, nr):
        row_share(k, me_row).start()
    row_parts[me_row] = col_parts[...]
    for k in range(1, nr):
        row_share(k, source(me_row, k, nr)).wait_recv()

    square = jnp.sum(row_parts[...].reshape(nr * n * 8, 128), keepdims=True)
    factor = jnp.minimum(F32(1.0), F32(limit) / (jnp.sqrt(square) + F32(1e-06)))
    factor = jnp.broadcast_to(factor, (8, cols))

    for c in range(chunks):
        m_load(c).wait()

        def update(r, carry, c=c):
            start = pl.multiple_of(c * step + r * 8, 8)
            for p in range(n):
                span = pl.ds(p * cols, cols)
                m = mbuf[c % 2, pl.ds(pl.multiple_of(r * 8, 8), 8), span]
                gbuf[pl.ds(start, 8), span] = F32(0.9) * m + factor * gbuf[pl.ds(start, 8), span]
            return carry

        lax.fori_loop(0, step // 8, update, 0)
        if c + 2 < chunks:
            m_load(c + 2).start()

    for k in routed:
        w_rest[k][0].wait_send()
    for k in direct + routed + near:
        nm_all[k][0].start()
    own_nm = pltpu.make_async_copy(gbuf.at[:, window(me)], nm_out.at[landing(me, 0, rows), :], own_sem.at[1])
    own_nm.start()
    for copy in tails:
        copy.start()

    for copy in tails:
        copy.wait()
    for k in peers:
        w_first[k][0].wait_send()
        if k not in routed:
            w_rest[k][0].wait_send()
        col_share(k, me).wait_send()
    for k in range(1, nr):
        row_share(k, me_row).wait_send()
    own_w.wait()
    own_nm.wait()
    for k in peers:
        w_first[k][1].wait_recv()
        w_rest[k][1].wait_recv()
    for k in peers:
        nm_all[k][0].wait_send()
        nm_all[k][1].wait_recv()


def finish(n, rows, tail, w_ref, nm_ref, nw_out, nm_out, buf, nw_sem, nm_sem):
    me = lax.axis_index("col")
    direct = kinds(n)[1]
    whole = pltpu.make_async_copy(nm_ref, nm_out, nm_sem)
    whole.start()
    writes = []
    for k in range(n):
        base = (source(me, k, n) if k else me) * rows
        size = rows - tail if k in direct else rows
        half = size // 16 * 8
        for start, count in ((0, half), (half, size - half)):

            def step(r, carry, base=base, start=start, k=k):
                here = pl.ds(pl.multiple_of(base + start + r * 8, 8), 8)
                kept = pl.ds(pl.multiple_of(k * rows + start + r * 8, 8), 8)
                buf[kept] = w_ref[here] - F32(0.1) * nm_ref[here]
                return carry

            lax.fori_loop(0, count // 8, step, 0)
            write = pltpu.make_async_copy(
                buf.at[pl.ds(k * rows + start, count)],
                nw_out.at[pl.ds(pl.multiple_of(base + start, 8), count)],
                nw_sem.at[len(writes)],
            )
            write.start()
            writes.append(write)
    whole.wait()
    for write in writes:
        write.wait()


def finish_tail(n, rows, tail, *refs):
    me = lax.axis_index("col")
    direct = kinds(n)[1]
    got_refs = refs[1 : 1 + len(direct)]
    nm_ref, nw_out, got, in_sem, out_sem = refs[1 + len(direct) :]
    loads = [pltpu.make_async_copy(ref, got.at[i], in_sem.at[i]) for i, ref in enumerate(got_refs)]
    for load in loads:
        load.start()
    writes = []
    for i, k in enumerate(direct):
        here = pl.ds(pl.multiple_of(source(me, k, n) * rows + rows - tail, 8), tail)
        loads[i].wait()
        got[i] = got[i] - F32(0.1) * nm_ref[here]
        write = pltpu.make_async_copy(got.at[i], nw_out.at[here], out_sem.at[i])
        write.start()
        writes.append(write)
    for write in writes:
        write.wait()


def body(n, nr, grad, momentum, weight):
    rows, width = grad.shape
    cols = width // n
    limit = math.sqrt(rows * n * nr * width)
    head = max(8, rows // 64 * 8)
    step = max(8, rows // 64 * 8)
    dma = pltpu.SemaphoreType.DMA
    anywhere, vmem = pl.BlockSpec(memory_space=pl.ANY), pl.BlockSpec(memory_space=pltpu.VMEM)
    local = rows * width * 4
    tail = min(TAIL, rows // 16 * 8)
    direct = kinds(n)[1]
    w_new, nm_new, *tails = pl.pallas_call(
        functools.partial(exchange, n, nr, limit, head, step, tail),
        out_shape=(pltpu.VMEM((n * rows, cols), F32),) * 2
        + (jax.ShapeDtypeStruct((tail, cols), F32),) * len(direct),
        in_specs=[anywhere] * 3,
        out_specs=(vmem,) * 2 + (anywhere,) * len(direct),
        scratch_shapes=[
            pltpu.VMEM((rows, width), F32),
            pltpu.VMEM((2, step, width), F32),
            pltpu.VMEM((8, 128), F32),
            pltpu.VMEM((n, 8, 128), F32),
            pltpu.VMEM((nr, n, 8, 128), F32),
            dma((rows // step,)), dma((2,)), dma((2,)), dma((len(direct),)),
            dma((n, 2)), dma((n, 2)), dma((n, 1)), dma((n, 1)),
            dma((n,)), dma((n,)), dma((nr,)), dma((nr,)),
        ],
        compiler_params=pltpu.CompilerParams(
            collective_id=0, has_side_effects=True,
            vmem_limit_bytes=local + 2 * step * width * 4 + 2 * MIB,
        ),
        name="exchange",
    )(grad, momentum, weight)
    turned = n & (n - 1) == 0
    got = [
        lax.ppermute(x, "col", [(d, d ^ k if turned else (d + k) % n) for d in range(n)])
        for k, x in zip(direct, tails)
    ]
    nw, nm = pl.pallas_call(
        functools.partial(finish, n, rows, tail),
        out_shape=(jax.ShapeDtypeStruct((n * rows, cols), F32),) * 2,
        in_specs=[vmem] * 2,
        out_specs=(anywhere,) * 2,
        scratch_shapes=[pltpu.VMEM((n * rows, cols), F32), dma((2 * n,)), dma],
        compiler_params=pltpu.CompilerParams(vmem_limit_bytes=local + 2 * MIB),
        cost_estimate=pl.CostEstimate(flops=2 * rows * width, bytes_accessed=2 * local, transcendentals=0),
        name="finish",
    )(w_new, nm_new)
    nw = pl.pallas_call(
        functools.partial(finish_tail, n, rows, tail),
        out_shape=jax.ShapeDtypeStruct((n * rows, cols), F32),
        in_specs=[anywhere] * (1 + len(direct)) + [vmem],
        out_specs=anywhere,
        scratch_shapes=[pltpu.VMEM((len(direct), tail, cols), F32), dma((len(direct),)), dma((len(direct),))],
        input_output_aliases={0: 0},
        compiler_params=pltpu.CompilerParams(vmem_limit_bytes=len(direct) * tail * cols * 4 + 2 * MIB),
        name="finish_tail",
    )(nw, *got, nm_new)
    return nw, nm


def solution(mesh):
    n, nr = mesh.shape["col"], mesh.shape["row"]
    spread = P(("row", "col"), None)
    return jax.shard_map(
        functools.partial(body, n, nr),
        mesh=mesh,
        in_specs=(spread,) * 3,
        out_specs=(P("row", "col"),) * 2,
        check_vma=False,
    )
```
